512 devices in a mesh: seq: 8 (over z), head: 4 (over x_hi, core), ctx: 16 (over y, x_lo).
Axes of the slice: x: 4 (x_hi: 2, x_lo: 2; x = x_hi * 2 + x_lo), y: 8, z: 8, core: 2. Of those that a mesh axis runs over, the one named last changes fastest.
Arguments:
- q_new: bfloat16 [4096, 8192], P('seq', ('head', 'ctx')), may hold values from -6 to 6
- k_prefix: bfloat16 [4096, 1024], P('seq', 'head'), may hold values from -204 to 204
- v_prefix: bfloat16 [4096, 1024], P('seq', 'head'), may hold values from -6 to 6
- k_new: bfloat16 [4096, 1024], P('seq', 'head'), may hold values from -204 to 204
- v_new: bfloat16 [4096, 1024], P('seq', 'head'), may hold values from -6 to 6
- block_offsets: int32 [32], P('seq'), may hold values from 0 to 2047
- dec_hidden: bfloat16 [256, 8192], P(None, 'ctx'), may hold values from -6 to 6
- w_query: bfloat16 [8192, 4, 2048], P('ctx', 'head', 'seq'), may hold values from -0.0625 to 0.0625
- w_out: bfloat16 [4, 2048, 8192], P('head', 'seq', 'ctx'), may hold values from -0.0625 to 0.0625
- k_own: bfloat16 [256, 1024], P(None, 'head'), may hold values from -21 to 21
- v_own: bfloat16 [256, 1024], P(None, 'head'), may hold values from -6 to 6
- valid_len: int32 [256], replicated, may hold values from 1 to 4096
- parent: int32 [256], replicated, may hold values from 0 to 4095
Outputs:
- prefill_out: bfloat16 [4096, 8192], P('seq', ('head', 'ctx'))
- decoded: bfloat16 [256, 8192], P(('seq', 'head'), 'ctx')
The draws below stay inside these ranges and needn't reach their ends.
All inputs are finite; a program needn't handle non-finite values.
Results may differ from the reference program's by a relative error of at most 0.017.
The reference program's roundings to bfloat16 on the way count: a program that leaves them out, or rounds other values in their place, can miss the bound.
Values may be sent and summed in bfloat16 or wider, within the bound.
No kernel may reach another device: no remote copies, remote signals or barrier semaphores. Data moves between devices by JAX's collectives and lax.ppermute only.
A program may use at most 64 MiB of HBM per device.

```python
import math
import jax
import jax.numpy as jnp
from jax import lax

D = 8192
HQ = 64
KVH = 8
HD = 128
ROWS = 256
QBLK = 128
PREFIX = 4096
NEW = 4096
GROUPS = 4


def spiky_keys(key, count, salt):
    base_key = jax.random.fold_in(key, 11 + salt)
    base = jax.random.truncated_normal(base_key, -6.0, 6.0, (count, KVH * HD), jnp.float32)
    return base.astype(jnp.bfloat16)


def draw_k_prefix(key, part):
    return spiky_keys(key, PREFIX, 0)


def draw_k_new(key, part):
    return spiky_keys(key, NEW, 101)


def plant(entries, stream_key, least, largest):
    shape = entries.shape
    index_at = [jax.random.randint(jax.random.fold_in(stream_key, axis), (), 0, shape[axis]) for axis in range(len(shape))]
    entries = entries.at[tuple(index_at)].set(least)
    longest = shape.index(max(shape))
    index_at[longest] = (index_at[longest] + 1) % shape[longest]
    return entries.at[tuple(index_at)].set(largest)


def level_of(own_key, extent, cuts, low, high):
    def one(axis_at, blocks):
        draws = jax.random.uniform(jax.random.fold_in(jax.random.fold_in(own_key, 6), axis_at), (blocks,), jnp.float32, low / len(cuts), high / len(cuts))
        return jnp.repeat(jnp.exp(draws), extent[axis_at] // blocks).reshape((-1,) + (1,) * (len(extent) - axis_at - 1))

    loudness = one(*cuts[0])
    for cut in cuts[1:]:
        loudness = loudness * one(*cut)
    return loudness


def scatter_about(stream_key, dims, scale, reach, split=(), kind=jnp.bfloat16):
    loudness = level_of(stream_key, dims, split, -0.22, 0.18) if split else 1.0
    result = jax.random.normal(stream_key, dims, jnp.float32) * scale * loudness
    return jnp.minimum(jnp.maximum(result, -reach), reach).astype(kind)


def setup_inputs(seed: int = 0) -> dict:
    streams_of = jax.random.split(jax.random.key(seed), 14)
    return {
        "q_new": scatter_about(streams_of[0], (NEW, HQ * HD), 1.0, 6.0, ((0, 8), (1, 64))),
        "k_prefix": draw_k_prefix(jax.random.fold_in(streams_of[13], 71), 0),
        "v_prefix": scatter_about(streams_of[2], (PREFIX, KVH * HD), 1.0, 6.0, ((0, 8), (1, 4))),
        "k_new": draw_k_new(jax.random.fold_in(streams_of[13], 71), 0),
        "v_new": scatter_about(streams_of[4], (NEW, KVH * HD), 1.0, 6.0, ((0, 8), (1, 4))),
        "block_offsets": plant(jax.random.randint(streams_of[5], (NEW // QBLK,), 0, PREFIX // 2), jax.random.fold_in(streams_of[5], 1), 0, (PREFIX // 2) - 1).astype(jnp.int32),
        "dec_hidden": scatter_about(streams_of[6], (ROWS, D), 1.0, 6.0, ((1, 16),)),
        "w_query": scatter_about(streams_of[7], (D, GROUPS, HQ // GROUPS * HD), D ** -0.5, 0.0625, ((0, 16), (1, 4), (2, 8))),
        "w_out": scatter_about(streams_of[8], (GROUPS, HQ // GROUPS * HD, D), D ** -0.5, 0.0625, ((0, 4), (1, 8), (2, 16))),
        "k_own": scatter_about(streams_of[9], (ROWS, KVH * HD), 3.5, 21.0, ((1, 4),)),
        "v_own": scatter_about(streams_of[10], (ROWS, KVH * HD), 1.0, 6.0, ((1, 4),)),
        "valid_len": plant(jax.random.randint(streams_of[11], (ROWS,), 1, PREFIX + 1), jax.random.fold_in(streams_of[11], 1), 1, PREFIX).astype(jnp.int32),
        "parent": plant(jax.random.randint(streams_of[12], (ROWS,), 0, NEW), jax.random.fold_in(streams_of[12], 1), 0, NEW - 1).astype(jnp.int32),
    }


def reference(q_new, k_prefix, v_prefix, k_new, v_new, block_offsets, dec_hidden, w_query, w_out, k_own, v_own, valid_len, parent):
    group_size = HQ // KVH
    scale = 1.0 / math.sqrt(HD)
    total_len = PREFIX + NEW
    keys = jnp.concatenate([k_prefix, k_new], axis=0).astype(jnp.float32).reshape(total_len, KVH, HD)
    values = jnp.concatenate([v_prefix, v_new], axis=0).astype(jnp.float32).reshape(total_len, KVH, HD)
    positions = jnp.arange(total_len, dtype=jnp.int32)
    firsts = jnp.repeat(block_offsets, QBLK)

    def prefill_block(inputs):
        query_blk, index_blk, first_blk = inputs
        queries = query_blk.astype(jnp.float32).reshape(QBLK, KVH, group_size, HD)
        scores = jnp.einsum('qkgd,tkd->qkgt', queries, keys) * scale
        visible = (positions[None, :] < PREFIX) & (positions[None, :] >= first_blk[:, None]) | (positions[None, :] >= PREFIX) & (positions[None, :] - PREFIX <= index_blk[:, None])
        scores = jnp.where(visible[:, None, None, :], scores, -jnp.inf)
        top = lax.optimization_barrier(jnp.max(scores, axis=-1, keepdims=True))
        weights = jnp.exp(scores - top)
        denom = lax.optimization_barrier(jnp.sum(weights, axis=-1))
        rounded = lax.optimization_barrier(weights.astype(jnp.bfloat16)).astype(jnp.float32)
        out = jnp.einsum('qkgt,tkd->qkgd', rounded, values) / denom[..., None]
        return out.astype(jnp.bfloat16).reshape(QBLK, HQ * HD)
    nblk = NEW // QBLK
    prefill_out = lax.map(prefill_block, (q_new.reshape(nblk, QBLK, HQ * HD), jnp.arange(NEW, dtype=jnp.int32).reshape(nblk, QBLK), firsts.reshape(nblk, QBLK))).reshape(NEW, HQ * HD)
    queries_all = jnp.dot(dec_hidden, w_query.reshape(D, HQ * HD), preferred_element_type=jnp.float32).astype(jnp.bfloat16)
    row_blk = math.gcd(ROWS, 32)
    rblocks = ROWS // row_blk

    def decode_block(inputs):
        query_blk, own_k, own_v, length_blk, parent_blk = inputs
        queries = query_blk.astype(jnp.float32).reshape(row_blk, KVH, group_size, HD)
        ownk = own_k.astype(jnp.float32).reshape(row_blk, KVH, HD)
        ownv = own_v.astype(jnp.float32).reshape(row_blk, KVH, HD)
        scores = jnp.einsum('rkgd,tkd->rkgt', queries, keys) * scale
        visible = (positions[None, :] < PREFIX) & (positions[None, :] < length_blk[:, None]) | (positions[None, :] >= PREFIX) & (positions[None, :] - PREFIX <= parent_blk[:, None])
        scores = jnp.where(visible[:, None, None, :], scores, -jnp.inf)
        own_score = jnp.einsum('rkgd,rkd->rkg', queries, ownk) * scale
        top = jnp.maximum(lax.optimization_barrier(jnp.max(scores, axis=-1)), own_score)
        weights = jnp.exp(scores - top[..., None])
        own_w = jnp.exp(own_score - top)
        denom = lax.optimization_barrier(jnp.sum(weights, axis=-1)) + own_w
        rounded = lax.optimization_barrier(weights.astype(jnp.bfloat16)).astype(jnp.float32)
        own_r = lax.optimization_barrier(own_w.astype(jnp.bfloat16)).astype(jnp.float32)
        out = jnp.einsum('rkgt,tkd->rkgd', rounded, values) + own_r[..., None] * ownv[:, :, None, :]
        out = out / denom[..., None]
        return out.astype(jnp.bfloat16).reshape(row_blk, HQ * HD)
    attn = lax.map(decode_block, (queries_all.reshape(rblocks, row_blk, HQ * HD), k_own.reshape(rblocks, row_blk, KVH * HD), v_own.reshape(rblocks, row_blk, KVH * HD), valid_len.reshape(rblocks, row_blk), parent.reshape(rblocks, row_blk))).reshape(ROWS, HQ * HD)
    decoded = jnp.dot(attn, w_out.reshape(HQ * HD, D), preferred_element_type=jnp.float32).astype(jnp.bfloat16)
    return (prefill_out, decoded)
```

```python
import math

import jax
import jax.numpy as jnp
from jax import lax
from jax.experimental import pallas as pl
from jax.experimental.pallas import tpu as pltpu
from jax.sharding import Mesh
from jax.sharding import PartitionSpec as P

HQ = 64
KVH = 8
HD = 128
QBLK = 128
CTX = ("ctx_0", "ctx_1")
HEAD_CTX = ("head", "ctx_0", "ctx_1")
GROUP = HQ // KVH
SCALE = 1.0 / math.sqrt(HD)
SCALE2 = math.log2(math.e) / math.sqrt(HD)
MASKED = -1e30
FLOOR = -1e20

SMEM = pl.BlockSpec(memory_space=pltpu.SMEM)
VMEM = pl.BlockSpec(memory_space=pltpu.VMEM)


def cost(flops, moved, transcendentals=0):
    return pl.CostEstimate(flops=flops, bytes_accessed=moved, transcendentals=transcendentals)


def contract(a, b, dim_a, dim_b):
    return lax.dot_general(
        a, b, (((dim_a,), (dim_b,)), ((), ())), preferred_element_type=jnp.float32
    )


def pack_kernel(at_ref, kp, vp, kn, vn, kps, vps, kns, vns, rows_ref, span_ref):
    block = kp.shape[0]
    for n, ref in enumerate((kp, vp, kn, vn)):
        rows_ref[n * block : (n + 1) * block] = ref[...]

    @pl.when(at_ref[2] == 0)
    def _():
        span_ref[:block] = kps[...]
        span_ref[block:] = vps[...]

    @pl.when(at_ref[2] != 0)
    def _():
        span_ref[:block] = kns[...]
        span_ref[block:] = vns[...]


def pack(at, k_prefix, v_prefix, k_new, v_new):
    block = k_prefix.shape[0]
    arrays = (k_prefix, v_prefix, k_new, v_new)
    first = pl.BlockSpec((block, HD), lambda i, at: (0, at[0]))
    second = pl.BlockSpec((block, HD), lambda i, at: (0, at[1]))
    whole = lambda n: pl.BlockSpec((n * block, HD), lambda i, at: (0, 0))
    return pl.pallas_call(
        pack_kernel,
        grid_spec=pltpu.PrefetchScalarGridSpec(
            num_scalar_prefetch=1,
            grid=(1,),
            in_specs=[first] * 4 + [second] * 4,
            out_specs=[whole(4), whole(2)],
        ),
        out_shape=[
            jax.ShapeDtypeStruct((4 * block, HD), k_prefix.dtype),
            jax.ShapeDtypeStruct((2 * block, HD), k_prefix.dtype),
        ],
        cost_estimate=cost(1 << 20, 14 * block * HD * 2),
        name="pack",
    )(at, *arrays, *arrays)


def prefill_kernel(off_ref, seq_ref, q_ref, kv_ref, o_ref, m_ref, l_ref, acc_ref):
    src = pl.program_id(0)
    seq = seq_ref[0]
    rows = q_ref.shape[0]
    block = kv_ref.shape[1] // 4

    @pl.when(src == 0)
    def _():
        m_ref[...] = jnp.full_like(m_ref, FLOOR)
        l_ref[...] = jnp.zeros_like(l_ref)
        acc_ref[...] = jnp.zeros_like(acc_ref)

    def run(base, visible):
        keys = kv_ref[0, base : base + block]
        values = kv_ref[0, base + block : base + 2 * block]
        s = contract(keys, q_ref[...], 1, 1)
        if visible is not None:
            s = jnp.where(visible(), s, MASKED)
        m = m_ref[...]
        top = jnp.maximum(m, jnp.max(s, axis=0, keepdims=True))
        factor = jnp.exp2((m - top) * SCALE2)
        p = jnp.exp2((s - top) * SCALE2)
        m_ref[...] = top
        l_ref[...] = l_ref[...] * factor + jnp.sum(p, axis=0, keepdims=True)
        acc_ref[...] = acc_ref[...] * factor + contract(values, p.astype(jnp.bfloat16), 0, 0)

    def in_prefix():
        pos = src * block + lax.broadcasted_iota(jnp.int32, (block, rows), 0)
        part = lax.broadcasted_iota(jnp.int32, (1, rows), 1) // QBLK
        first = jnp.full((1, rows), off_ref[0], jnp.int32)
        for n in range(1, off_ref.shape[0]):
            first = jnp.where(part == n, off_ref[n], first)
        return pos >= first

    def causal():
        at = lax.broadcasted_iota(jnp.int32, (block, rows), 0)
        return at <= lax.broadcasted_iota(jnp.int32, (block, rows), 1)

    last = off_ref[0]
    for n in range(1, off_ref.shape[0]):
        last = jnp.maximum(last, off_ref[n])
    pl.when(src * block >= last)(lambda: run(0, None))
    pl.when(src * block < last)(lambda: run(0, in_prefix))
    pl.when(src < seq)(lambda: run(2 * block, None))
    pl.when(src == seq)(lambda: run(2 * block, causal))

    @pl.when(src == pl.num_programs(0) - 1)
    def _():
        o_ref[...] = jnp.transpose(acc_ref[...] / l_ref[...]).astype(o_ref.dtype)


def prefill(offsets, seq, q, cache):
    n, size, _ = cache.shape
    rows = q.shape[0]
    return pl.pallas_call(
        prefill_kernel,
        grid=(n,),
        out_shape=jax.ShapeDtypeStruct(q.shape, jnp.bfloat16),
        in_specs=[
            SMEM,
            SMEM,
            pl.BlockSpec((rows, HD), lambda i: (0, 0)),
            pl.BlockSpec((1, size, HD), lambda i: (i, 0, 0)),
        ],
        out_specs=pl.BlockSpec((rows, HD), lambda i: (0, 0)),
        scratch_shapes=[
            pltpu.VMEM((1, rows), jnp.float32),
            pltpu.VMEM((1, rows), jnp.float32),
            pltpu.VMEM((HD, rows), jnp.float32),
        ],
        compiler_params=pltpu.CompilerParams(dimension_semantics=("arbitrary",)),
        cost_estimate=cost(2 * rows * n * size * HD, n * size * HD * 2, rows * n * size // 2),
        name="prefill",
    )(offsets, seq, q, cache)


def sum_kernel(parts_ref, out_ref):
    total = jnp.sum(parts_ref[...], axis=0).astype(out_ref.dtype)
    for n in range(out_ref.shape[0]):
        out_ref[n] = total


def summed_for_all(parts):
    return pl.pallas_call(
        sum_kernel,
        out_shape=jax.ShapeDtypeStruct(parts.shape, jnp.bfloat16),
        in_specs=[VMEM],
        out_specs=VMEM,
        cost_estimate=cost(parts.size, parts.size * 6),
        name="sum_queries",
    )(parts)


def three_parts(x):
    high = x.astype(jnp.bfloat16)
    rest = x - high.astype(jnp.float32)
    middle = rest.astype(jnp.bfloat16)
    return (high, middle, (rest - middle.astype(jnp.float32)).astype(jnp.bfloat16))


def span_kernel(q_ref, span_ref, limit_ref, out_ref):
    rows = q_ref.shape[0]
    heads = q_ref.shape[1] // HD
    block = span_ref.shape[0] // 2
    keys, values = span_ref[:block], span_ref[block:]
    visible = lax.broadcasted_iota(jnp.int32, (rows, block), 1) < limit_ref[...]
    lane = lax.broadcasted_iota(jnp.int32, (rows, HD), 1)
    stats = jnp.zeros((rows, HD), jnp.float32)
    for h in range(heads):
        s = contract(q_ref[:, h * HD : (h + 1) * HD], keys, 1, 1)
        s = jnp.where(visible, s, MASKED)
        top = jnp.maximum(jnp.max(s, axis=1, keepdims=True), FLOOR)
        p = jnp.exp2((s - top) * SCALE2)
        total = jnp.sum(p, axis=1, keepdims=True)
        accum = contract(p.astype(jnp.bfloat16), values, 1, 0)
        out_ref[:, h * HD : (h + 1) * HD] = (
            accum / jnp.where(total > 0.0, total, 1.0)
        ).astype(out_ref.dtype)
        for n, part in enumerate(three_parts(top) + three_parts(total)):
            stats = jnp.where(lane == 6 * h + n, part.astype(jnp.float32), stats)
    out_ref[:, heads * HD :] = stats.astype(out_ref.dtype)


def span_attention(queries, span, limit):
    rows, width = queries.shape
    block = span.shape[0] // 2
    return pl.pallas_call(
        span_kernel,
        out_shape=jax.ShapeDtypeStruct((rows, width + HD), jnp.bfloat16),
        in_specs=[VMEM] * 3,
        out_specs=VMEM,
        cost_estimate=cost(4 * rows * width * block, (rows * width + block * HD) * 4),
        name="span_attention",
    )(queries, span, limit)


def merge_kernel(parts_ref, q_ref, k_ref, v_ref, out_ref):
    copies, rows, width = out_ref.shape
    heads = width // HD
    own_k = k_ref[...].astype(jnp.float32)
    own_v = v_ref[...].astype(jnp.float32)
    stats = parts_ref[:, :, width:].astype(jnp.float32)
    merged = []
    for h in range(heads):
        part = [stats[:, :, 6 * h + n : 6 * h + n + 1] for n in range(6)]
        tops = part[0] + part[1] + part[2]
        totals = part[3] + part[4] + part[5]
        q = q_ref[:, h * HD : (h + 1) * HD].astype(jnp.float32)
        own = jnp.sum(q * own_k, axis=1, keepdims=True)
        top = jnp.maximum(jnp.max(tops, axis=0), own)
        weights = jnp.exp2((tops - top[None]) * SCALE2) * totals
        own_w = jnp.exp2((own - top) * SCALE2)
        total = jnp.sum(weights, axis=0) + own_w
        values = parts_ref[:, :, h * HD : (h + 1) * HD].astype(jnp.float32)
        accum = jnp.sum(weights * values, axis=0)
        accum = accum + own_w.astype(jnp.bfloat16).astype(jnp.float32) * own_v
        merged.append((accum / total).astype(out_ref.dtype))
    whole = jnp.concatenate(merged, axis=1)
    for n in range(copies):
        out_ref[n] = whole


def merged_for_all(parts, queries, own_k, own_v):
    copies, rows, _ = parts.shape
    return pl.pallas_call(
        merge_kernel,
        out_shape=jax.ShapeDtypeStruct((copies, *queries.shape), jnp.bfloat16),
        in_specs=[VMEM] * 4,
        out_specs=VMEM,
        cost_estimate=cost(parts.size * 4, parts.size * 4),
        name="merge",
    )(parts, queries, own_k, own_v)


def body(
    q_new,
    k_prefix,
    v_prefix,
    k_new,
    v_new,
    block_offsets,
    dec_hidden,
    w_query,
    w_out,
    k_own,
    v_own,
    valid_len,
    parent,
):
    n_seq = lax.axis_size("seq")
    n_ctx = lax.axis_size(CTX)
    seq = lax.axis_index("seq")
    ctx = lax.axis_index(CTX)
    block = q_new.shape[0]
    rows = dec_hidden.shape[0]
    heads_dec = w_query.shape[2] // HD
    width = heads_dec * HD
    chunk = rows // n_ctx

    for_seq = ctx % n_seq
    at = jnp.stack([ctx // GROUP, for_seq * heads_dec // GROUP, ctx // n_seq]).astype(jnp.int32)
    mine, span = pack(at, k_prefix, v_prefix, k_new, v_new)
    partial_q = jnp.dot(
        dec_hidden, w_query.reshape(w_query.shape[0], -1), preferred_element_type=jnp.float32
    )
    parts = lax.all_to_all(partial_q.reshape(n_ctx, chunk, width), CTX, 0, 0, tiled=True)
    cache = lax.all_gather(mine, "seq")
    span = lax.ppermute(
        span,
        ("seq", *CTX),
        [
            ((c % n_seq) * n_ctx + s + n_seq * (c // n_seq), s * n_ctx + c)
            for s in range(n_seq)
            for c in range(n_ctx)
        ]
        if n_ctx == 2 * n_seq
        else None,
    )
    my_q = summed_for_all(parts)
    dec_q = lax.all_to_all(my_q, CTX, 0, 0, tiled=True).reshape(rows, width)
    limit = jnp.where(
        ctx < n_seq, valid_len - ctx * block, parent + 1 - (ctx - n_seq) * block
    ).reshape(rows, 1)
    local = span_attention(dec_q, span, limit)
    parts = lax.all_to_all(local.reshape(n_ctx, chunk, width + HD), CTX, 0, 0, tiled=True)
    kv_dec = seq * heads_dec // GROUP
    own_k = lax.dynamic_slice(k_own, (ctx * chunk, kv_dec * HD), (chunk, HD))
    own_v = lax.dynamic_slice(v_own, (ctx * chunk, kv_dec * HD), (chunk, HD))
    attn = merged_for_all(parts, my_q[0], own_k, own_v)
    attn = lax.all_to_all(attn, CTX, 0, 0, tiled=True).reshape(rows, width)
    summed = jnp.dot(
        attn, w_out.reshape(-1, w_out.shape[2]), preferred_element_type=jnp.float32
    ).astype(jnp.bfloat16)
    devices = lax.axis_size(("seq", "head"))
    tiles = lax.all_to_all(
        summed.reshape(devices, rows // devices, -1), ("seq", "head"), 0, 0, tiled=True
    )
    decoded = jnp.sum(tiles.astype(jnp.float32), axis=0).astype(jnp.bfloat16)
    prefill_out = prefill(block_offsets, seq.reshape(1).astype(jnp.int32), q_new, cache)
    return (prefill_out, decoded)


def solution(mesh):
    split = Mesh(
        mesh.devices.reshape(mesh.shape["seq"], mesh.shape["head"], 8, 2),
        ("seq", "head", "ctx_0", "ctx_1"),
    )
    return jax.shard_map(
        body,
        mesh=split,
        in_specs=(
            P("seq", HEAD_CTX),
            P("seq", "head"),
            P("seq", "head"),
            P("seq", "head"),
            P("seq", "head"),
            P("seq"),
            P(None, CTX),
            P(CTX, "head", "seq"),
            P("head", "seq", CTX),
            P(None, "head"),
            P(None, "head"),
            P(),
            P(),
        ),
        out_specs=(P("seq", HEAD_CTX), P(("seq", "head"), CTX)),
        check_vma=False,
    )
```

```python
import math

import jax
import jax.numpy as jnp
from jax import lax
from jax.experimental import pallas as pl
from jax.experimental.pallas import tpu as pltpu
from jax.sharding import Mesh
from jax.sharding import PartitionSpec as P

HQ = 64
KVH = 8
HD = 128
QBLK = 128
CTX = ("ctx_0", "ctx_1")
HEAD_CTX = ("head", "ctx_0", "ctx_1")
GROUP = HQ // KVH
SCALE2 = math.log2(math.e) / math.sqrt(HD)
MASKED = -1e30
FLOOR = -1e20

SMEM = pl.BlockSpec(memory_space=pltpu.SMEM)
VMEM = pl.BlockSpec(memory_space=pltpu.VMEM)


def cost(flops, moved, transcendentals=0):
    return pl.CostEstimate(flops=flops, bytes_accessed=moved, transcendentals=transcendentals)


def contract(a, b, dim_a, dim_b):
    return lax.dot_general(
        a, b, (((dim_a,), (dim_b,)), ((), ())), preferred_element_type=jnp.float32
    )


def pack_kernel(at_ref, kp, vp, kn, vn, rows_ref):
    block = kp.shape[0]
    for n, ref in enumerate((kp, vp, kn, vn)):
        rows_ref[n * block : (n + 1) * block] = ref[...]


def pack(at, k_prefix, v_prefix, k_new, v_new):
    block = k_prefix.shape[0]
    return pl.pallas_call(
        pack_kernel,
        grid_spec=pltpu.PrefetchScalarGridSpec(
            num_scalar_prefetch=1,
            grid=(1,),
            in_specs=[pl.BlockSpec((block, HD), lambda i, at: (0, at[0]))] * 4,
            out_specs=pl.BlockSpec((4 * block, HD), lambda i, at: (0, 0)),
        ),
        out_shape=jax.ShapeDtypeStruct((4 * block, HD), k_prefix.dtype),
        cost_estimate=cost(1 << 20, 8 * block * HD * 2),
        name="pack",
    )(at, k_prefix, v_prefix, k_new, v_new)


def prefill_kernel(off_ref, seq_ref, q_ref, kv_ref, o_ref, m_ref, l_ref, acc_ref):
    src = pl.program_id(0)
    seq = seq_ref[0]
    rows = q_ref.shape[0]
    block = kv_ref.shape[1] // 4

    @pl.when(src == 0)
    def _():
        m_ref[...] = jnp.full_like(m_ref, FLOOR)
        l_ref[...] = jnp.zeros_like(l_ref)
        acc_ref[...] = jnp.zeros_like(acc_ref)

    def run(base, visible):
        keys = kv_ref[0, base : base + block]
        values = kv_ref[0, base + block : base + 2 * block]
        s = contract(keys, q_ref[...], 1, 1)
        if visible is not None:
            s = jnp.where(visible(), s, MASKED)
        m = m_ref[...]
        top = jnp.maximum(m, jnp.max(s, axis=0, keepdims=True))
        factor = jnp.exp2((m - top) * SCALE2)
        p = jnp.exp2((s - top) * SCALE2)
        m_ref[...] = top
        l_ref[...] = l_ref[...] * factor + jnp.sum(p, axis=0, keepdims=True)
        acc_ref[...] = acc_ref[...] * factor + contract(values, p.astype(jnp.bfloat16), 0, 0)

    def in_prefix():
        pos = src * block + lax.broadcasted_iota(jnp.int32, (block, rows), 0)
        part = lax.broadcasted_iota(jnp.int32, (1, rows), 1) // QBLK
        first = jnp.full((1, rows), off_ref[0], jnp.int32)
        for n in range(1, off_ref.shape[0]):
            first = jnp.where(part == n, off_ref[n], first)
        return pos >= first

    def causal():
        at = lax.broadcasted_iota(jnp.int32, (block, rows), 0)
        return at <= lax.broadcasted_iota(jnp.int32, (block, rows), 1)

    last = off_ref[0]
    for n in range(1, off_ref.shape[0]):
        last = jnp.maximum(last, off_ref[n])
    pl.when(src * block >= last)(lambda: run(0, None))
    pl.when(src * block < last)(lambda: run(0, in_prefix))
    pl.when(src < seq)(lambda: run(2 * block, None))
    pl.when(src == seq)(lambda: run(2 * block, causal))

    @pl.when(src == pl.num_programs(0) - 1)
    def _():
        o_ref[...] = jnp.transpose(acc_ref[...] / l_ref[...]).astype(o_ref.dtype)


def prefill(offsets, seq, q, cache):
    n, size, _ = cache.shape
    rows = q.shape[0]
    return pl.pallas_call(
        prefill_kernel,
        grid=(n,),
        out_shape=jax.ShapeDtypeStruct(q.shape, jnp.bfloat16),
        in_specs=[
            SMEM,
            SMEM,
            pl.BlockSpec((rows, HD), lambda i: (0, 0)),
            pl.BlockSpec((1, size, HD), lambda i: (i, 0, 0)),
        ],
        out_specs=pl.BlockSpec((rows, HD), lambda i: (0, 0)),
        scratch_shapes=[
            pltpu.VMEM((1, rows), jnp.float32),
            pltpu.VMEM((1, rows), jnp.float32),
            pltpu.VMEM((HD, rows), jnp.float32),
        ],
        compiler_params=pltpu.CompilerParams(dimension_semantics=("arbitrary",)),
        cost_estimate=cost(2 * rows * n * size * HD, n * size * HD * 2, rows * n * size // 2),
        name="prefill",
    )(offsets, seq, q, cache)


def sum_kernel(parts_ref, out_ref):
    total = jnp.sum(parts_ref[...], axis=0).astype(out_ref.dtype)
    for n in range(out_ref.shape[0]):
        out_ref[n] = total


def summed_for_all(parts, copies):
    return pl.pallas_call(
        sum_kernel,
        out_shape=jax.ShapeDtypeStruct((copies, *parts.shape[1:]), jnp.bfloat16),
        in_specs=[VMEM],
        out_specs=VMEM,
        cost_estimate=cost(parts.size, parts.size * 6),
        name="sum_queries",
    )(parts)


def three_parts(x):
    high = x.astype(jnp.bfloat16)
    rest = x - high.astype(jnp.float32)
    middle = rest.astype(jnp.bfloat16)
    return (high, middle, (rest - middle.astype(jnp.float32)).astype(jnp.bfloat16))


def rows_kernel(q_ref, kp_ref, vp_ref, kn_ref, vn_ref, limit_ref, out_ref):
    owners, chunk, width = q_ref.shape
    heads = width // HD
    cached = kp_ref.shape[1] // HD
    near = owners // cached
    block = kp_ref.shape[0]
    count = near * heads * chunk
    lane = lax.broadcasted_iota(jnp.int32, (chunk, HD), 1)
    at = lax.broadcasted_iota(jnp.int32, (count, block), 1)
    limits = jnp.concatenate([limit_ref[...]] * (near * heads), axis=0)
    for kv in range(cached):
        cols = slice(kv * HD, (kv + 1) * HD)
        q = jnp.concatenate(
            [
                q_ref[owner, :, h * HD : (h + 1) * HD]
                for owner in range(kv * near, (kv + 1) * near)
                for h in range(heads)
            ],
            axis=0,
        )
        s = [
            jnp.where(at < limits[:, n : n + 1], contract(q, keys[:, cols], 1, 1), MASKED)
            for n, keys in enumerate((kp_ref, kn_ref))
        ]
        top = jnp.maximum(
            jnp.maximum(
                jnp.max(s[0], axis=1, keepdims=True), jnp.max(s[1], axis=1, keepdims=True)
            ),
            FLOOR,
        )
        p = [jnp.exp2((x - top) * SCALE2) for x in s]
        total = jnp.sum(p[0], axis=1, keepdims=True) + jnp.sum(p[1], axis=1, keepdims=True)
        accum = contract(p[0].astype(jnp.bfloat16), vp_ref[:, cols], 1, 0) + contract(
            p[1].astype(jnp.bfloat16), vn_ref[:, cols], 1, 0
        )
        values = accum / jnp.where(total > 0.0, total, 1.0)
        parts = three_parts(top) + three_parts(total)
        for n in range(near):
            stats = jnp.zeros((chunk, HD), jnp.float32)
            for h in range(heads):
                here = slice((n * heads + h) * chunk, (n * heads + h + 1) * chunk)
                out_ref[kv * near + n, :, h * HD : (h + 1) * HD] = values[here].astype(
                    out_ref.dtype
                )
                for k, part in enumerate(parts):
                    stats = jnp.where(lane == 6 * h + k, part[here].astype(jnp.float32), stats)
            out_ref[kv * near + n, :, width:] = stats.astype(out_ref.dtype)


def rows_attention(queries, k_prefix, v_prefix, k_new, v_new, limit):
    owners, chunk, width = queries.shape
    block = k_prefix.shape[0]
    return pl.pallas_call(
        rows_kernel,
        out_shape=jax.ShapeDtypeStruct((owners, chunk, width + HD), jnp.bfloat16),
        in_specs=[VMEM] * 6,
        out_specs=VMEM,
        cost_estimate=cost(8 * queries.size * block, k_prefix.size * 8),
        name="rows_attention",
    )(queries, k_prefix, v_prefix, k_new, v_new, limit)


def merge_kernel(at_ref, parts_ref, q_ref, k_ref, v_ref, out_ref):
    copies, _, width = out_ref.shape
    heads = width // HD
    own_k = k_ref[...].astype(jnp.float32)
    own_v = v_ref[...].astype(jnp.float32)
    stats = parts_ref[:, :, width:].astype(jnp.float32)
    merged = []
    for h in range(heads):
        part = [stats[:, :, 6 * h + n : 6 * h + n + 1] for n in range(6)]
        tops = part[0] + part[1] + part[2]
        totals = part[3] + part[4] + part[5]
        q = q_ref[0, :, h * HD : (h + 1) * HD].astype(jnp.float32)
        own = jnp.sum(q * own_k, axis=1, keepdims=True)
        top = jnp.maximum(jnp.max(tops, axis=0), own)
        weights = jnp.exp2((tops - top[None]) * SCALE2) * totals
        own_w = jnp.exp2((own - top) * SCALE2)
        total = jnp.sum(weights, axis=0) + own_w
        values = parts_ref[:, :, h * HD : (h + 1) * HD].astype(jnp.float32)
        accum = jnp.sum(weights * values, axis=0)
        accum = accum + own_w.astype(jnp.bfloat16).astype(jnp.float32) * own_v
        merged.append((accum / total).astype(out_ref.dtype))
    whole = jnp.concatenate(merged, axis=1)
    for n in range(copies):
        out_ref[n] = whole


def merged_for_all(at, parts, queries, k_own, v_own, copies):
    sources, chunk, width = parts.shape
    own = pl.BlockSpec((chunk, HD), lambda i, at: (at[1], at[2]))
    return pl.pallas_call(
        merge_kernel,
        grid_spec=pltpu.PrefetchScalarGridSpec(
            num_scalar_prefetch=1,
            grid=(1,),
            in_specs=[
                pl.BlockSpec((sources, chunk, width), lambda i, at: (0, 0, 0)),
                pl.BlockSpec((1, chunk, width - HD), lambda i, at: (0, 0, 0)),
                own,
                own,
            ],
            out_specs=pl.BlockSpec((copies, chunk, width - HD), lambda i, at: (0, 0, 0)),
        ),
        out_shape=jax.ShapeDtypeStruct((copies, chunk, width - HD), jnp.bfloat16),
        cost_estimate=cost(parts.size * 4, parts.size * 4),
        name="merge",
    )(at, parts, queries, k_own, v_own)


def body(
    q_new,
    k_prefix,
    v_prefix,
    k_new,
    v_new,
    block_offsets,
    dec_hidden,
    w_query,
    w_out,
    k_own,
    v_own,
    valid_len,
    parent,
):
    n_seq = lax.axis_size("seq")
    n_ctx = lax.axis_size(CTX)
    seq = lax.axis_index("seq")
    ctx = lax.axis_index(CTX)
    block = q_new.shape[0]
    rows = dec_hidden.shape[0]
    heads_dec = w_query.shape[2] // HD
    width = heads_dec * HD
    chunk = rows // n_ctx

    at = jnp.stack([ctx // GROUP, ctx, seq * heads_dec // GROUP]).astype(jnp.int32)
    mine = pack(at, k_prefix, v_prefix, k_new, v_new)
    cache = lax.all_gather(mine, "seq")

    partial_q = jnp.dot(
        dec_hidden, w_query.reshape(w_query.shape[0], -1), preferred_element_type=jnp.float32
    )
    parts = lax.all_to_all(partial_q.reshape(n_ctx, chunk, width), CTX, 0, 0, tiled=True)
    my_q = summed_for_all(parts, n_seq)
    dec_q = lax.all_to_all(my_q, "seq", 0, 0, tiled=True)
    limit = jnp.stack([valid_len, parent + 1], axis=1) - seq * block
    limit = lax.dynamic_slice_in_dim(limit, ctx * chunk, chunk, 0)
    local = rows_attention(dec_q, k_prefix, v_prefix, k_new, v_new, limit)
    parts = lax.all_to_all(local, "seq", 0, 0, tiled=True)
    attn = merged_for_all(at, parts, my_q, k_own, v_own, n_ctx)
    attn = lax.all_to_all(attn, CTX, 0, 0, tiled=True).reshape(rows, width)
    summed = jnp.dot(
        attn, w_out.reshape(-1, w_out.shape[2]), preferred_element_type=jnp.float32
    ).astype(jnp.bfloat16)
    devices = lax.axis_size(("seq", "head"))
    tiles = lax.all_to_all(
        summed.reshape(devices, rows // devices, -1), ("seq", "head"), 0, 0, tiled=True
    )
    decoded = jnp.sum(tiles.astype(jnp.float32), axis=0).astype(jnp.bfloat16)
    prefill_out = prefill(block_offsets, seq.reshape(1).astype(jnp.int32), q_new, cache)
    return (prefill_out, decoded)


def solution(mesh):
    split = Mesh(
        mesh.devices.reshape(mesh.shape["seq"], mesh.shape["head"], 8, 2),
        ("seq", "head", "ctx_0", "ctx_1"),
    )
    return jax.shard_map(
        body,
        mesh=split,
        in_specs=(
            P("seq", HEAD_CTX),
            P("seq", "head"),
            P("seq", "head"),
            P("seq", "head"),
            P("seq", "head"),
            P("seq"),
            P(None, CTX),
            P(CTX, "head", "seq"),
            P("head", "seq", CTX),
            P(None, "head"),
            P(None, "head"),
            P(),
            P(),
        ),
        out_specs=(P("seq", HEAD_CTX), P(("seq", "head"), CTX)),
        check_vma=False,
    )
```
